8 devices in a mesh: dp: 2 (over z, y), tp: 4 (over x, core).
Axes of the slice: x: 2, y: 2, z: 1, core: 2. Of those that a mesh axis runs over, the one named last changes fastest.
Arguments:
- hidden: bfloat16 [1024, 4096], P('dp'), parts along dimension 0
- w_q: bfloat16 [4096, 4096], P(None, 'tp')
- w_k: bfloat16 [4096, 4096], P(None, 'tp')
- w_v: bfloat16 [4096, 4096], P(None, 'tp')
- w_o: bfloat16 [4096, 4096], P('tp')
- q_norm_w: float32 [4096], P('tp')
- k_norm_w: float32 [4096], P('tp')
- post_norm_w: float32 [4096], replicated
- k_cache: bfloat16 [1024, 32, 32, 128], P('dp', None, 'tp'), parts along dimension 0
- v_cache: bfloat16 [1024, 32, 32, 128], P('dp', None, 'tp'), parts along dimension 0
- positions: int32 [1024], P('dp'), parts along dimension 0
Outputs:
- output 1: bfloat16 [1024, 4096], P('dp'), parts along dimension 0
- output 2: bfloat16 [1024, 32, 32, 128], P('dp', None, 'tp'), parts along dimension 0
- output 3: bfloat16 [1024, 32, 32, 128], P('dp', None, 'tp'), parts along dimension 0
There are 2 independent parts. The reference program is written for one: setup_inputs(seed, part) draws one part's arguments, and reference() takes and returns one part's arrays. A program takes and returns all parts, laid end to end along the dimension named above; an argument that names none is the same for every part.
All inputs are finite; a program needn't handle non-finite values.
Results may differ from the reference program's by a relative error of at most 0.010336.
Values are sent between devices in bfloat16 or wider.
A program may use at most 1 GiB of HBM per device.

```python
import jax
import jax.numpy as jnp
from jax import lax

BATCH = 512
CACHE_LEN = 32
HEADS = 32
HEAD_DIM = 128
WIDTH = HEADS * HEAD_DIM
NORM_EPS = 1e-6
ROPE_BASE = 500000.0


def setup_inputs(seed: int = 0, part: int = 0) -> dict:
    base_key = jax.random.key(seed)
    shared_keys = jax.random.split(base_key, 9)
    part_keys = jax.random.split(jax.random.fold_in(base_key, part), 6)
    fan_scale = WIDTH ** -0.5
    head_frac = jnp.arange(HEADS, dtype=jnp.float32) / max(HEADS - 1, 1)
    q_heads = jnp.exp(1.2 * (2.0 * head_frac - 1.0) + 0.2 * jax.random.normal(shared_keys[0], (HEADS,)))
    k_heads = jnp.exp(1.2 * (1.0 - 2.0 * head_frac) + 0.2 * jax.random.normal(shared_keys[1], (HEADS,)))
    q_cols = jnp.repeat(q_heads, HEAD_DIM)
    k_cols = jnp.repeat(k_heads, HEAD_DIM)
    w_q = (jax.random.normal(shared_keys[2], (WIDTH, WIDTH)) * fan_scale * q_cols[None, :]).astype(jnp.bfloat16)
    w_k = (jax.random.normal(shared_keys[3], (WIDTH, WIDTH)) * fan_scale * k_cols[None, :]).astype(jnp.bfloat16)
    w_v = (jax.random.normal(shared_keys[4], (WIDTH, WIDTH)) * fan_scale).astype(jnp.bfloat16)
    w_o = (jax.random.normal(shared_keys[5], (WIDTH, WIDTH)) * fan_scale).astype(jnp.bfloat16)
    q_norm_w = jax.random.uniform(shared_keys[6], (WIDTH,), minval=0.5, maxval=1.5).astype(jnp.float32)
    k_norm_w = jax.random.uniform(shared_keys[7], (WIDTH,), minval=0.5, maxval=1.5).astype(jnp.float32)
    post_norm_w = jax.random.uniform(shared_keys[8], (WIDTH,), minval=0.5, maxval=1.5).astype(jnp.float32)
    hidden = jax.random.normal(part_keys[0], (BATCH, WIDTH)).astype(jnp.bfloat16)
    k_cache = jax.random.normal(part_keys[1], (BATCH, CACHE_LEN, HEADS, HEAD_DIM)).astype(jnp.bfloat16)
    v_cache = jax.random.normal(part_keys[2], (BATCH, CACHE_LEN, HEADS, HEAD_DIM)).astype(jnp.bfloat16)
    slot_draw = jax.random.randint(part_keys[3], (BATCH,), 0, CACHE_LEN, dtype=jnp.int32)
    shift_bits = jax.random.randint(part_keys[4], (BATCH,), 0, 10, dtype=jnp.int32)
    longest = jax.random.randint(part_keys[5], (), 0, BATCH, dtype=jnp.int32)
    positions = jnp.where(jnp.arange(BATCH, dtype=jnp.int32) == longest, CACHE_LEN - 1, jnp.right_shift(slot_draw, shift_bits)).astype(jnp.int32)
    return dict(hidden=hidden, w_q=w_q, w_k=w_k, w_v=w_v, w_o=w_o, q_norm_w=q_norm_w, k_norm_w=k_norm_w, post_norm_w=post_norm_w, k_cache=k_cache, v_cache=v_cache, positions=positions)


def width_norm(vals, gain):
    wide = vals.astype(jnp.float32)
    inv_rms = lax.rsqrt(jnp.mean(wide * wide, axis=-1, keepdims=True) + NORM_EPS)
    return wide * inv_rms * gain


def apply_rope(heads_val, positions):
    half = HEAD_DIM // 2
    inv_freq = ROPE_BASE ** (-2.0 * jnp.arange(half, dtype=jnp.float32) / HEAD_DIM)
    angles = positions.astype(jnp.float32)[:, None, None] * inv_freq[None, None, :]
    cos_tab = jnp.cos(angles)
    sin_tab = jnp.sin(angles)
    wide = heads_val.astype(jnp.float32)
    first = wide[..., :half]
    second = wide[..., half:]
    return jnp.concatenate([first * cos_tab - second * sin_tab, second * cos_tab + first * sin_tab], axis=-1).astype(jnp.bfloat16)


def attend_row(row_args):
    q_row, k_row, v_row, row_pos = row_args
    slot_ids = jnp.arange(CACHE_LEN)
    scores = jnp.einsum('hd,shd->hs', q_row.astype(jnp.float32), k_row.astype(jnp.float32)) * HEAD_DIM ** -0.5
    scores = jnp.where(slot_ids[None, :] <= row_pos, scores, -1e30)
    probs = jax.nn.softmax(scores, axis=-1).astype(jnp.bfloat16)
    return jnp.einsum('hs,shd->hd', probs.astype(jnp.float32), v_row.astype(jnp.float32)).astype(jnp.bfloat16)


def reference(hidden, w_q, w_k, w_v, w_o, q_norm_w, k_norm_w, post_norm_w, k_cache, v_cache, positions):
    n_rows = hidden.shape[0]
    q_full = jnp.dot(hidden, w_q, preferred_element_type=jnp.float32).astype(jnp.bfloat16)
    k_full = jnp.dot(hidden, w_k, preferred_element_type=jnp.float32).astype(jnp.bfloat16)
    v_full = jnp.dot(hidden, w_v, preferred_element_type=jnp.float32).astype(jnp.bfloat16)
    q_normed = width_norm(q_full, q_norm_w).astype(jnp.bfloat16).reshape(n_rows, HEADS, HEAD_DIM)
    k_normed = width_norm(k_full, k_norm_w).astype(jnp.bfloat16).reshape(n_rows, HEADS, HEAD_DIM)
    q_rot = apply_rope(q_normed, positions)
    k_rot = apply_rope(k_normed, positions)
    v_heads = v_full.reshape(n_rows, HEADS, HEAD_DIM)
    at_slot = (jnp.arange(CACHE_LEN)[None, :] == positions[:, None])[:, :, None, None]
    k_new = jnp.where(at_slot, k_rot[:, None], k_cache)
    v_new = jnp.where(at_slot, v_heads[:, None], v_cache)
    attn = lax.map(attend_row, (q_rot, k_new, v_new, positions))
    a_out = jnp.dot(attn.reshape(n_rows, WIDTH), w_o, preferred_element_type=jnp.float32)
    hidden_out = (hidden.astype(jnp.float32) + width_norm(a_out, post_norm_w)).astype(jnp.bfloat16)
    return hidden_out, k_new, v_new
```

```python
import functools

import jax
import jax.numpy as jnp
from jax import lax
from jax.experimental import pallas as pl
from jax.experimental.pallas import tpu as pltpu
from jax.sharding import PartitionSpec as P


NORM_EPS = 1e-6
ROPE_BASE = 500000.0
CHUNKS = (64,) * 8
BLOCK = 8
DEPTH = 6
AHEAD = 3
FINAL_ROWS = 16
PARTNER = [(0, 1), (1, 0), (2, 3), (3, 2)]
PEER = [(0, 2), (2, 0), (1, 3), (3, 1)]

VMEM = pl.BlockSpec(memory_space=pltpu.VMEM)
SMEM = pl.BlockSpec(memory_space=pltpu.SMEM)
ANY = pl.BlockSpec(memory_space=pl.ANY)


def attend_kernel(row0, rows, *refs):
    pos, core, q, kn, vn, wo, kc, vc = refs[:8]
    ko, vo, keep, send, kbuf, vbuf, o_f32, o_bf, isem, osem = refs[-10:]
    blocks = rows // BLOCK
    heads, dim = q.shape[1], q.shape[2]
    slots = kc.shape[1]

    def copies_in(j, s):
        at = pl.ds(row0 + j * BLOCK, BLOCK)
        return (pltpu.make_async_copy(kc.at[at], kbuf.at[s], isem.at[s, 0]),
                pltpu.make_async_copy(vc.at[at], vbuf.at[s], isem.at[s, 1]))

    def copies_out(j, s):
        at = pl.ds(row0 + j * BLOCK, BLOCK)
        return (pltpu.make_async_copy(kbuf.at[s], ko.at[at], osem.at[s, 0]),
                pltpu.make_async_copy(vbuf.at[s], vo.at[at], osem.at[s, 1]))

    for j in range(min(AHEAD, blocks)):
        for c in copies_in(j, j):
            c.start()

    lane = lax.broadcasted_iota(jnp.int32, (heads, slots * heads), 1)
    head = lax.broadcasted_iota(jnp.int32, (heads, slots * heads), 0)
    slot_of = jnp.where(lax.rem(lane, heads) == head, lax.div(lane, heads), slots)

    def step(i, carry):
        s = lax.rem(i, DEPTH)
        nxt = i + AHEAD

        @pl.when(nxt < blocks)
        def _():
            @pl.when(nxt >= DEPTH)
            def _():
                for c in copies_out(nxt - DEPTH, lax.rem(nxt, DEPTH)):
                    c.wait()

            for c in copies_in(nxt, lax.rem(nxt, DEPTH)):
                c.start()

        for c in copies_in(i, s):
            c.wait()
        base = i * BLOCK
        for r in range(BLOCK):
            p = pos[row0 + base + r]
            kbuf[s, r, p] = kn[row0 + base + r]
            vbuf[s, r, p] = vn[row0 + base + r]
        for r in range(BLOCK):
            p = pos[row0 + base + r]
            k = kbuf[s, r].reshape(slots * heads, dim)
            v = vbuf[s, r].reshape(slots * heads, dim)
            score = lax.dot_general(q[row0 + base + r], k, (((1,), (1,)), ((), ())), preferred_element_type=jnp.float32)
            score = jnp.where(slot_of <= p, score * dim ** -0.5, -1e30)
            e = jnp.exp(score - jnp.max(score, axis=-1, keepdims=True))
            prob = (e / jnp.sum(e, axis=-1, keepdims=True)).astype(jnp.bfloat16)
            o_f32[pl.ds((base + r) * heads, heads)] = jnp.dot(prob, v, preferred_element_type=jnp.float32)
        for c in copies_out(i, s):
            c.start()
        return carry

    lax.fori_loop(0, blocks, step, 0)
    for h in range(heads):
        o_bf[:, h * dim:(h + 1) * dim] = o_f32[pl.ds(h, rows, stride=heads), :].astype(jnp.bfloat16)
    half = rows // 2
    for which, out in ((core[0], keep), (1 - core[0], send)):
        o = o_bf[pl.ds(pl.multiple_of(which * half, 16), half), :]
        for n in range(0, wo.shape[1], 512):
            out[:, n:n + 512] = jnp.dot(o, wo[:, n:n + 512], preferred_element_type=jnp.float32).astype(jnp.bfloat16)
    for j in range(max(0, blocks - DEPTH), blocks):
        for c in copies_out(j, j % DEPTH):
            c.wait()


def attend(row0, rows, pos, core, q, kn, vn, wo, kc, vc, prev):
    width = wo.shape[1]
    args = (pos, core, q, kn, vn, wo, kc, vc) + prev
    share = jax.ShapeDtypeStruct((rows // 2, width), jnp.bfloat16)
    return pl.pallas_call(
        functools.partial(attend_kernel, row0, rows),
        out_shape=(jax.ShapeDtypeStruct(kc.shape, kc.dtype), jax.ShapeDtypeStruct(vc.shape, vc.dtype), share, share),
        in_specs=[SMEM, SMEM, VMEM, VMEM, VMEM, VMEM, ANY, ANY] + [ANY] * len(prev),
        out_specs=(ANY, ANY, VMEM, VMEM),
        input_output_aliases={8: 0, 9: 1} if prev else {},
        scratch_shapes=[
            pltpu.VMEM((DEPTH, BLOCK) + kc.shape[1:], kc.dtype),
            pltpu.VMEM((DEPTH, BLOCK) + vc.shape[1:], vc.dtype),
            pltpu.VMEM((rows * q.shape[1], q.shape[2]), jnp.float32),
            pltpu.VMEM((rows, q.shape[1] * q.shape[2]), jnp.bfloat16),
            pltpu.SemaphoreType.DMA((DEPTH, 2)),
            pltpu.SemaphoreType.DMA((DEPTH, 2)),
        ],
        compiler_params=pltpu.CompilerParams(vmem_limit_bytes=32 * 2 ** 20),
        cost_estimate=pl.CostEstimate(flops=rows * 75_000_000, bytes_accessed=rows * 4 * 65536, transcendentals=0),
        name='attend',
    )(*args)


def final_kernel(core, hid, own, peer, own2, peer2, gain, *rest):
    out = rest[-1]
    j = pl.program_id(0)

    def emit(a, b):
        total = a[...].astype(jnp.float32) + b[...].astype(jnp.float32)
        inv = lax.rsqrt(jnp.mean(total * total, axis=-1, keepdims=True) + NORM_EPS)
        out[...] = (hid[...].astype(jnp.float32) + total * inv * gain[...]).astype(jnp.bfloat16)

    @pl.when(j == 0)
    def _():
        emit(own, peer)

    @pl.when(j == 1)
    def _():
        emit(own2, peer2)


def finish(row0, rows, core, hidden, own, peer, own2, peer2, gain, prev):
    width = hidden.shape[1]
    blocks = rows // 2 // FINAL_ROWS
    first = row0 // FINAL_ROWS

    def place(j, b, core):
        which = core[0] + j - 2 * core[0] * j
        return (first + which * blocks + b, 0)

    mine = pl.BlockSpec((FINAL_ROWS, width), lambda j, b, core: (b + j * (blocks - 1 - b), 0))
    other = pl.BlockSpec((FINAL_ROWS, width), lambda j, b, core: (b * j, 0))
    return pl.pallas_call(
        final_kernel,
        out_shape=jax.ShapeDtypeStruct(hidden.shape, hidden.dtype),
        grid_spec=pltpu.PrefetchScalarGridSpec(
            num_scalar_prefetch=1,
            grid=(2, blocks),
            in_specs=[pl.BlockSpec((FINAL_ROWS, width), place), mine, mine, other, other,
                      pl.BlockSpec((1, width), lambda j, b, core: (0, 0))] + [ANY] * len(prev),
            out_specs=pl.BlockSpec((FINAL_ROWS, width), place),
        ),
        input_output_aliases={7: 0} if prev else {},
        compiler_params=pltpu.CompilerParams(vmem_limit_bytes=8 * 2 ** 20),
        cost_estimate=pl.CostEstimate(flops=rows * 8_000_000, bytes_accessed=rows * 32768, transcendentals=0),
        name='finish',
    )(core, hidden, own, peer, own2, peer2, gain, *prev)


def apply_rope(heads_val, positions):
    head_dim = heads_val.shape[-1]
    half = head_dim // 2
    inv_freq = ROPE_BASE ** (-2.0 * jnp.arange(half, dtype=jnp.float32) / head_dim)
    angles = positions.astype(jnp.float32)[:, None, None] * inv_freq[None, None, :]
    cos_tab = jnp.cos(angles)
    sin_tab = jnp.sin(angles)
    wide = heads_val.astype(jnp.float32)
    first = wide[..., :half]
    second = wide[..., half:]
    return jnp.concatenate([first * cos_tab - second * sin_tab, second * cos_tab + first * sin_tab], axis=-1).astype(jnp.bfloat16)


def solution(mesh):
    def local_step(hidden, w_q, w_k, w_v, w_o, q_norm_w, k_norm_w, post_norm_w, k_cache, v_cache, positions):
        n_rows, width = hidden.shape
        local_heads, head_dim = k_cache.shape[2], k_cache.shape[3]
        q_local = jnp.dot(hidden, w_q, preferred_element_type=jnp.float32).astype(jnp.bfloat16).astype(jnp.float32)
        k_local = jnp.dot(hidden, w_k, preferred_element_type=jnp.float32).astype(jnp.bfloat16).astype(jnp.float32)
        v_local = jnp.dot(hidden, w_v, preferred_element_type=jnp.float32).astype(jnp.bfloat16)
        energy = jnp.stack([jnp.sum(q_local * q_local, axis=-1), jnp.sum(k_local * k_local, axis=-1)])
        energy = lax.psum(energy, 'tp')
        inv_rms = lax.rsqrt(energy / width + NORM_EPS)
        q_normed = (q_local * inv_rms[0][:, None] * q_norm_w).astype(jnp.bfloat16).reshape(n_rows, local_heads, head_dim)
        k_normed = (k_local * inv_rms[1][:, None] * k_norm_w).astype(jnp.bfloat16).reshape(n_rows, local_heads, head_dim)
        q_rot = apply_rope(q_normed, positions)
        k_rot = apply_rope(k_normed, positions)
        v_new = v_local.reshape(n_rows, local_heads, head_dim)
        core = jnp.reshape(lax.rem(lax.axis_index('tp'), 2), (1,)).astype(jnp.int32)
        gain = post_norm_w.reshape(1, width)

        caches, out, row0 = (), (), 0
        for rows in CHUNKS:
            k_out, v_out, keep, send = attend(row0, rows, positions, core, q_rot, k_rot, v_new, w_o, k_cache, v_cache, caches)
            caches = (k_out, v_out)
            got = lax.ppermute(send, 'tp', PARTNER)
            own = (keep.astype(jnp.float32) + got.astype(jnp.float32)).astype(jnp.bfloat16)
            peer = lax.ppermute(own, 'tp', PEER)
            own2 = lax.ppermute(own, 'tp', PARTNER)
            peer2 = lax.ppermute(peer, 'tp', PARTNER)
            out = (finish(row0, rows, core, hidden, own, peer, own2, peer2, gain, out),)
            row0 += rows
        return out[0], caches[0], caches[1]

    cache_spec = P('dp', None, 'tp', None)
    return jax.shard_map(local_step, mesh=mesh, in_specs=(P('dp', None), P(None, 'tp'), P(None, 'tp'), P(None, 'tp'), P('tp', None), P('tp'), P('tp'), P(None), cache_spec, cache_spec, P('dp')), out_specs=(P('dp', None), cache_spec, cache_spec), check_vma=False)
```

```python
import functools

import jax
import jax.numpy as jnp
from jax import lax
from jax.experimental import pallas as pl
from jax.experimental.pallas import tpu as pltpu
from jax.sharding import PartitionSpec as P


NORM_EPS = 1e-6
ROPE_BASE = 500000.0
CHUNKS = (160, 128, 128, 96)
BLOCK = 8
DEPTH = 10
FINAL_ROWS = 16
PARTNER = [(0, 1), (1, 0), (2, 3), (3, 2)]
PEER = [(0, 2), (2, 0), (1, 3), (3, 1)]

VMEM = pl.BlockSpec(memory_space=pltpu.VMEM)
SMEM = pl.BlockSpec(memory_space=pltpu.SMEM)
ANY = pl.BlockSpec(memory_space=pl.ANY)


def attend_kernel(row0, rows, *refs):
    pos, core, q, kn, vn, wo, kc, vc = refs[:8]
    ko, vo, parts, kbuf, vbuf, o_f32, o_bf, isem, osem = refs[-9:]
    blocks = rows // BLOCK
    depth = kbuf.shape[0]
    ahead = depth - 3
    heads, dim = q.shape[1], q.shape[2]
    slots = kc.shape[1]
    span = slots * heads

    def copies_in(j, s):
        at = pl.ds(row0 + j * BLOCK, BLOCK)
        return (pltpu.make_async_copy(kc.at[at], kbuf.at[s], isem.at[s, 0]),
                pltpu.make_async_copy(vc.at[at], vbuf.at[s], isem.at[s, 1]))

    def copies_out(j, s):
        at = pl.ds(row0 + j * BLOCK, BLOCK)
        return (pltpu.make_async_copy(kbuf.at[s], ko.at[at], osem.at[s, 0]),
                pltpu.make_async_copy(vbuf.at[s], vo.at[at], osem.at[s, 1]))

    for j in range(min(ahead, blocks)):
        for c in copies_in(j, j):
            c.start()

    lane = lax.broadcasted_iota(jnp.int32, (heads, span), 1)
    head = lax.broadcasted_iota(jnp.int32, (heads, span), 0)
    slot_of = jnp.where(lax.rem(lane, heads) == head, lax.div(lane, heads), slots)

    def arrive(i):
        s = lax.rem(i, depth)
        for c in copies_in(i, s):
            c.wait()
        for r in range(BLOCK):
            row = row0 + i * BLOCK + r
            p = pos[row]
            kbuf[s, r, p] = kn[row]
            vbuf[s, r, p] = vn[row]

    def scores(i):
        s = lax.rem(i, depth)
        out = []
        for r in range(BLOCK):
            row = row0 + i * BLOCK + r
            k = kbuf[s, r].reshape(span, dim)
            score = lax.dot_general(q[row], k, (((1,), (1,)), ((), ())), preferred_element_type=jnp.float32)
            out.append(jnp.where(slot_of <= pos[row], score * dim ** -0.5, -1e30))
        return jnp.concatenate(out, axis=0)

    def softmax(score):
        e = jnp.exp(score - jnp.max(score, axis=-1, keepdims=True))
        return (e / jnp.sum(e, axis=-1, keepdims=True)).astype(jnp.bfloat16)

    def mix(i, prob):
        s = lax.rem(i, depth)
        for r in range(BLOCK):
            v = vbuf[s, r].reshape(span, dim)
            at = pl.ds((i * BLOCK + r) * heads, heads)
            o_f32[at] = jnp.dot(prob[r * heads:(r + 1) * heads], v, preferred_element_type=jnp.float32)
        for c in copies_out(i, s):
            c.start()

    arrive(0)

    def step(i, score):
        nxt = i - 1 + ahead

        @pl.when(nxt < blocks)
        def _():
            @pl.when(nxt >= depth)
            def _():
                for c in copies_out(nxt - depth, lax.rem(nxt, depth)):
                    c.wait()

            for c in copies_in(nxt, lax.rem(nxt, depth)):
                c.start()

        arrive(i)
        prob = softmax(score)
        new = scores(i)
        mix(i - 1, prob)
        return new

    last = lax.fori_loop(1, blocks, step, scores(0))
    mix(blocks - 1, softmax(last))
    for h in range(heads):
        o_bf[:, h * dim:(h + 1) * dim] = o_f32[pl.ds(h, rows, stride=heads), :].astype(jnp.bfloat16)
    half = rows // 2
    for j, which in ((0, core[0]), (1, 1 - core[0])):
        o = o_bf[pl.ds(pl.multiple_of(which * half, 16), half), :]
        for n in range(0, wo.shape[1], 512):
            parts[j, :, n:n + 512] = jnp.dot(o, wo[:, n:n + 512], preferred_element_type=jnp.float32).astype(jnp.bfloat16)
    for j in range(max(0, blocks - depth), blocks):
        for c in copies_out(j, j % depth):
            c.wait()


def attend(row0, rows, pos, core, q, kn, vn, wo, kc, vc, prev):
    width = wo.shape[1]
    args = (pos, core, q, kn, vn, wo, kc, vc) + prev
    share = jax.ShapeDtypeStruct((2, rows // 2, width), jnp.bfloat16)
    return pl.pallas_call(
        functools.partial(attend_kernel, row0, rows),
        out_shape=(jax.ShapeDtypeStruct(kc.shape, kc.dtype), jax.ShapeDtypeStruct(vc.shape, vc.dtype), share),
        in_specs=[SMEM, SMEM, VMEM, VMEM, VMEM, VMEM, ANY, ANY] + [ANY] * len(prev),
        out_specs=(ANY, ANY, VMEM),
        input_output_aliases={8: 0, 9: 1} if prev else {},
        scratch_shapes=[
            pltpu.VMEM((DEPTH, BLOCK) + kc.shape[1:], kc.dtype),
            pltpu.VMEM((DEPTH, BLOCK) + vc.shape[1:], vc.dtype),
            pltpu.VMEM((rows * q.shape[1], q.shape[2]), jnp.float32),
            pltpu.VMEM((rows, q.shape[1] * q.shape[2]), jnp.bfloat16),
            pltpu.SemaphoreType.DMA((DEPTH, 2)),
            pltpu.SemaphoreType.DMA((DEPTH, 2)),
        ],
        compiler_params=pltpu.CompilerParams(vmem_limit_bytes=32 * 2 ** 20),
        cost_estimate=pl.CostEstimate(flops=rows * 75_000_000, bytes_accessed=rows * 4 * 65536, transcendentals=0),
        name='attend',
    )(*args)


def final_kernel(core, hid, own, peer, mine, got, peer2, gain, *rest):
    out = rest[-1]
    j = pl.program_id(0)

    def emit(a, b):
        total = a + b[...].astype(jnp.float32)
        inv = lax.rsqrt(jnp.mean(total * total, axis=-1, keepdims=True) + NORM_EPS)
        out[...] = (hid[...].astype(jnp.float32) + total * inv * gain[...]).astype(jnp.bfloat16)

    @pl.when(j == 0)
    def _():
        emit(own[...].astype(jnp.float32), peer)

    @pl.when(j == 1)
    def _():
        chip = (mine[...].astype(jnp.float32) + got[...].astype(jnp.float32)).astype(jnp.bfloat16)
        emit(chip.astype(jnp.float32), peer2)


def finish(row0, rows, core, hidden, own, peer, parts, got, peer2, gain, prev):
    width = hidden.shape[1]
    blocks = rows // 2 // FINAL_ROWS
    first = row0 // FINAL_ROWS

    def place(j, b, core):
        which = core[0] + j - 2 * core[0] * j
        return (first + which * blocks + b, 0)

    def early(j, b, core):
        return (b + j * (blocks - 1 - b), 0)

    def late(j, b, core):
        return (b * j, 0)

    block = (FINAL_ROWS, width)
    return pl.pallas_call(
        final_kernel,
        out_shape=jax.ShapeDtypeStruct(hidden.shape, hidden.dtype),
        grid_spec=pltpu.PrefetchScalarGridSpec(
            num_scalar_prefetch=1,
            grid=(2, blocks),
            in_specs=[
                pl.BlockSpec(block, place), pl.BlockSpec(block, early), pl.BlockSpec(block, early),
                pl.BlockSpec((None,) + block, lambda j, b, core: (1,) + late(j, b, core)),
                pl.BlockSpec((None,) + block, lambda j, b, core: (0,) + late(j, b, core)),
                pl.BlockSpec(block, late), pl.BlockSpec((1, width), lambda j, b, core: (0, 0)),
            ] + [ANY] * len(prev),
            out_specs=pl.BlockSpec(block, place),
        ),
        input_output_aliases={8: 0} if prev else {},
        compiler_params=pltpu.CompilerParams(vmem_limit_bytes=8 * 2 ** 20),
        cost_estimate=pl.CostEstimate(flops=rows * 8_000_000, bytes_accessed=rows * 32768, transcendentals=0),
        name='finish',
    )(core, hidden, own, peer, parts, got, peer2, gain, *prev)


def apply_rope(heads_val, positions):
    head_dim = heads_val.shape[-1]
    half = head_dim // 2
    inv_freq = ROPE_BASE ** (-2.0 * jnp.arange(half, dtype=jnp.float32) / head_dim)
    angles = positions.astype(jnp.float32)[:, None, None] * inv_freq[None, None, :]
    cos_tab = jnp.cos(angles)
    sin_tab = jnp.sin(angles)
    wide = heads_val.astype(jnp.float32)
    first = wide[..., :half]
    second = wide[..., half:]
    return jnp.concatenate([first * cos_tab - second * sin_tab, second * cos_tab + first * sin_tab], axis=-1).astype(jnp.bfloat16)


def solution(mesh):
    def local_step(hidden, w_q, w_k, w_v, w_o, q_norm_w, k_norm_w, post_norm_w, k_cache, v_cache, positions):
        n_rows, width = hidden.shape
        local_heads, head_dim = k_cache.shape[2], k_cache.shape[3]
        q_local = jnp.dot(hidden, w_q, preferred_element_type=jnp.float32).astype(jnp.bfloat16).astype(jnp.float32)
        k_local = jnp.dot(hidden, w_k, preferred_element_type=jnp.float32).astype(jnp.bfloat16).astype(jnp.float32)
        v_local = jnp.dot(hidden, w_v, preferred_element_type=jnp.float32).astype(jnp.bfloat16)
        energy = jnp.stack([jnp.sum(q_local * q_local, axis=-1), jnp.sum(k_local * k_local, axis=-1)])
        energy = lax.psum(energy, 'tp')
        inv_rms = lax.rsqrt(energy / width + NORM_EPS)
        q_normed = (q_local * inv_rms[0][:, None] * q_norm_w).astype(jnp.bfloat16).reshape(n_rows, local_heads, head_dim)
        k_normed = (k_local * inv_rms[1][:, None] * k_norm_w).astype(jnp.bfloat16).reshape(n_rows, local_heads, head_dim)
        q_rot = apply_rope(q_normed, positions)
        k_rot = apply_rope(k_normed, positions)
        v_new = v_local.reshape(n_rows, local_heads, head_dim)
        core = jnp.reshape(lax.rem(lax.axis_index('tp'), 2), (1,)).astype(jnp.int32)
        gain = post_norm_w.reshape(1, width)

        caches, out, row0 = (), (), 0
        for rows in CHUNKS:
            k_out, v_out, parts = attend(row0, rows, positions, core, q_rot, k_rot, v_new, w_o, k_cache, v_cache, caches)
            caches = (k_out, v_out)
            got = lax.ppermute(parts, 'tp', PARTNER)
            own = (parts[0].astype(jnp.float32) + got[1].astype(jnp.float32)).astype(jnp.bfloat16)
            peer = lax.ppermute(own, 'tp', PEER)
            peer2 = lax.ppermute(peer, 'tp', PARTNER)
            out = (finish(row0, rows, core, hidden, own, peer, parts, got, peer2, gain, out),)
            row0 += rows
        return out[0], caches[0], caches[1]

    cache_spec = P('dp', None, 'tp', None)
    return jax.shard_map(local_step, mesh=mesh, in_specs=(P('dp', None), P(None, 'tp'), P(None, 'tp'), P(None, 'tp'), P('tp', None), P('tp'), P('tp'), P(None), cache_spec, cache_spec, P('dp')), out_specs=(P('dp', None), cache_spec, cache_spec), check_vma=False)
```
